32 devices in a mesh: patch: 8 (over z, y), hidden: 4 (over x, core).
Axes of the slice: x: 2, y: 2, z: 4, core: 2. Of those that a mesh axis runs over, the one named last changes fastest.
Arguments:
- grid_latent: bfloat16 [24576, 512], P('patch'), may hold values from -6 to 6
- mesh_latent: bfloat16 [40960, 512], P('patch'), may hold values from -6 to 6
- edge_latent: bfloat16 [65536, 512], P('patch'), may hold values from -6 to 6
- senders: int32 [65536], P('patch'), may hold values from 0 to 24575, as said below
- receivers: int32 [65536], P('patch'), may hold values from 0 to 40959
- mesh_slot: int32 [40960], replicated, may hold values from 0 to 40959, as said below
- edge_counts: int32 [8], P('patch'), may hold values from 2730 to 8192, as said below
- w_edge: bfloat16 [512, 512], P(None, 'hidden'), may hold values from -0.25 to 0.25
- w_sender: bfloat16 [512, 512], P(None, 'hidden'), may hold values from -0.25 to 0.25
- w_receiver: bfloat16 [512, 512], P(None, 'hidden'), may hold values from -0.25 to 0.25
- edge_bias: float32 [512], P('hidden'), may hold values from -3 to 3
- w_edge_out: bfloat16 [512, 512], P('hidden'), may hold values from -0.25 to 0.25
- edge_out_bias: float32 [512], P('hidden'), may hold values from -3 to 3
- edge_gain: float32 [512], P('hidden'), may hold values from 0.25 to 1.75
- edge_shift: float32 [512], P('hidden'), may hold values from -2 to 2
- w_mesh_in: bfloat16 [512, 512], P(None, 'hidden'), may hold values from -0.25 to 0.25
- w_message_in: bfloat16 [512, 512], P(None, 'hidden'), may hold values from -0.25 to 0.25
- mesh_bias: float32 [512], P('hidden'), may hold values from -3 to 3
- w_mesh_out: bfloat16 [512, 512], P('hidden'), may hold values from -0.25 to 0.25
- mesh_out_bias: float32 [512], P('hidden'), may hold values from -3 to 3
- mesh_gain: float32 [512], P('hidden'), may hold values from 0.25 to 1.75
- mesh_shift: float32 [512], P('hidden'), may hold values from -2 to 2
Outputs:
- mesh_out: bfloat16 [40960, 512], P('patch', 'hidden')
- edge_out: bfloat16 [65536, 512], P('patch', 'hidden')
The draws below stay inside these ranges and needn't reach their ends.
Inputs may be any that keep to these rules, and one draw needn't show every extreme that they name: `mesh_slot`: A permutation of the mesh node ids 0 to 40959; owner block p holds mesh rows p * 5120 to (p + 1) * 5120 - 1. `senders`: edge slots of block p (slots p * 8192 to (p + 1) * 8192 - 1) send from grid nodes p * 3072 to (p + 1) * 3072 - 1. Only the first edge_counts[p] slots of block p are live; some block is full.
All inputs are finite; a program needn't handle non-finite values.
Results may differ from the reference program's by a relative error of at most 0.014.
Values may be sent and summed in bfloat16 or wider, within the bound.
A program may use at most 192 MiB of HBM per device.

```python
import jax
import jax.numpy as jnp
from jax import lax

LATENT = 512
G_DEV = 3072
E_DEV = 8192
MESH_DEV = 5120
GRID = 24576
EDGES = 65536
MESH = 40960
N_HIDDEN = 4


def mesh_order(key):
    return jax.random.permutation(jax.random.fold_in(key, 11), MESH).astype(jnp.int32)


def draw_mesh_slot(key, part):
    return mesh_order(key)


def draw_receivers(key, part):
    order = mesh_order(key)
    inverse = jnp.argsort(order, stable=True).astype(jnp.int32)
    first, second = jax.random.split(jax.random.fold_in(key, 12))
    third = jax.random.fold_in(key, 15)
    position = jnp.arange(EDGES, dtype=jnp.int32)
    blocks = EDGES // E_DEV
    pick = jax.random.randint(first, (EDGES,), 0, 8)
    anywhere = jax.random.randint(third, (EDGES,), 0, blocks).astype(jnp.int32)
    offset = jnp.where(pick == 4, -1, jnp.where(pick == 7, 1, 0)).astype(jnp.int32)
    nearby = (position // E_DEV + offset + blocks) % blocks
    owner = jnp.where(pick < 4, anywhere, nearby).astype(jnp.int32)
    target = owner * MESH_DEV + jax.random.randint(second, (EDGES,), 0, MESH_DEV)
    return jnp.take(inverse, target).astype(jnp.int32)


def draw_senders(key, part):
    position = jnp.arange(EDGES, dtype=jnp.int32)
    local = jax.random.randint(jax.random.fold_in(key, 13), (EDGES,), 0, G_DEV)
    return (position // E_DEV * G_DEV + local).astype(jnp.int32)


def draw_edge_counts(key, part):
    first, second = jax.random.split(jax.random.fold_in(key, 14))
    blocks = EDGES // E_DEV
    counts = jax.random.randint(first, (blocks,), E_DEV // 3, E_DEV + 1)
    fullest = jax.random.randint(second, (), 0, blocks)
    return jnp.where(jnp.arange(blocks) == fullest, E_DEV, counts).astype(jnp.int32)


def steps_of(own_key, extent, shards, smallest, high):
    level, own = 1.0, jax.random.fold_in(own_key, 6)
    for axis_at, shards_of in shards:
        heights = jnp.exp(jax.random.uniform(jax.random.fold_in(own, axis_at), (shards_of,), jnp.float32, smallest / len(shards), high / len(shards)))
        level = level * jnp.repeat(heights, extent[axis_at] // shards_of).reshape([-1 if axis == axis_at else 1 for axis in range(len(extent))])
    return level


def bell_draw(rng, extent, scale, most, shards=(), held_as=jnp.bfloat16):
    entries = scale * jax.random.normal(rng, extent, jnp.float32)
    if shards:
        entries = entries * steps_of(rng, extent, shards, -0.22, 0.18)
    return jnp.clip(entries, -most, most).astype(held_as)


def setup_inputs(seed: int = 0) -> dict:
    key_list = jax.random.split(jax.random.key(seed), 23)
    return {
        "grid_latent": bell_draw(key_list[0], (GRID, LATENT), 1.0, 6.0, ((0, 8),)),
        "mesh_latent": bell_draw(key_list[1], (MESH, LATENT), 1.0, 6.0, ((0, 8),)),
        "edge_latent": bell_draw(key_list[2], (EDGES, LATENT), 1.0, 6.0, ((0, 8),)),
        "senders": draw_senders(jax.random.fold_in(key_list[22], 71), 0),
        "receivers": draw_receivers(jax.random.fold_in(key_list[22], 71), 0),
        "mesh_slot": draw_mesh_slot(jax.random.fold_in(key_list[22], 71), 0),
        "edge_counts": draw_edge_counts(jax.random.fold_in(key_list[22], 71), 0),
        "w_edge": bell_draw(key_list[7], (LATENT, LATENT), LATENT ** -0.5, 0.25, ((1, 4),)),
        "w_sender": bell_draw(key_list[8], (LATENT, LATENT), LATENT ** -0.5, 0.25, ((1, 4),)),
        "w_receiver": bell_draw(key_list[9], (LATENT, LATENT), LATENT ** -0.5, 0.25, ((1, 4),)),
        "edge_bias": bell_draw(key_list[10], (LATENT,), 0.5, 3.0, ((0, 4),), jnp.float32),
        "w_edge_out": bell_draw(key_list[11], (LATENT, LATENT), LATENT ** -0.5, 0.25, ((0, 4),)),
        "edge_out_bias": bell_draw(key_list[12], (LATENT,), 0.5, 3.0, ((0, 4),), jnp.float32),
        "edge_gain": jnp.clip(1.0 + 0.15 * jax.random.normal(key_list[13], (LATENT,), jnp.float32), 0.25, 1.75),
        "edge_shift": bell_draw(key_list[14], (LATENT,), 0.3, 2.0, ((0, 4),), jnp.float32),
        "w_mesh_in": bell_draw(key_list[15], (LATENT, LATENT), LATENT ** -0.5, 0.25, ((1, 4),)),
        "w_message_in": bell_draw(key_list[16], (LATENT, LATENT), LATENT ** -0.5, 0.25, ((1, 4),)),
        "mesh_bias": bell_draw(key_list[17], (LATENT,), 0.5, 3.0, ((0, 4),), jnp.float32),
        "w_mesh_out": bell_draw(key_list[18], (LATENT, LATENT), LATENT ** -0.5, 0.25, ((0, 4),)),
        "mesh_out_bias": bell_draw(key_list[19], (LATENT,), 0.5, 3.0, ((0, 4),), jnp.float32),
        "mesh_gain": jnp.clip(1.0 + 0.15 * jax.random.normal(key_list[20], (LATENT,), jnp.float32), 0.25, 1.75),
        "mesh_shift": bell_draw(key_list[21], (LATENT,), 0.3, 2.0, ((0, 4),), jnp.float32),
    }


def group_sum(hidden_units, w_out):
    width = w_out.shape[0] // N_HIDDEN
    total = jnp.zeros((hidden_units.shape[0], w_out.shape[1]), jnp.float32)
    for group in range(N_HIDDEN):
        part = jnp.dot(hidden_units[:, group * width:(group + 1) * width], w_out[group * width:(group + 1) * width], preferred_element_type=jnp.float32)
        part = lax.optimization_barrier(part.astype(jnp.bfloat16))
        total = total + part.astype(jnp.float32)
    return total

def normalize(values, gain, offset):
    center = lax.optimization_barrier(jnp.mean(values, axis=1, keepdims=True))
    centered = values - center
    spread = lax.optimization_barrier(jnp.mean(centered * centered, axis=1, keepdims=True))
    return centered * lax.rsqrt(spread + 1e-05) * gain + offset

def reference(grid_latent, mesh_latent, edge_latent, senders, receivers, mesh_slot, edge_counts, w_edge, w_sender, w_receiver, edge_bias, w_edge_out, edge_out_bias, edge_gain, edge_shift, w_mesh_in, w_message_in, mesh_bias, w_mesh_out, mesh_out_bias, mesh_gain, mesh_shift):
    target = jnp.take(mesh_slot, receivers).astype(jnp.int32)
    position = jnp.arange(EDGES, dtype=jnp.int32)
    live = (position % E_DEV < jnp.take(edge_counts, position // E_DEV)).astype(jnp.float32)
    receiver_proj = jnp.dot(mesh_latent, w_receiver, preferred_element_type=jnp.float32).astype(jnp.bfloat16)
    sender_proj = jnp.dot(grid_latent, w_sender, preferred_element_type=jnp.float32)
    edge_pre = jnp.dot(edge_latent, w_edge, preferred_element_type=jnp.float32)
    edge_pre = edge_pre + jnp.take(sender_proj, senders, axis=0) + jnp.take(receiver_proj, target, axis=0).astype(jnp.float32) + edge_bias
    edge_hidden = jax.nn.silu(edge_pre).astype(jnp.bfloat16)
    edge_sum = group_sum(edge_hidden, w_edge_out) + edge_out_bias
    message = normalize(edge_sum, edge_gain, edge_shift) * live[:, None]
    edge_out = (edge_latent.astype(jnp.float32) + message).astype(jnp.bfloat16)
    summed = jax.ops.segment_sum(message, target, num_segments=MESH).astype(jnp.bfloat16)
    mesh_pre = jnp.dot(mesh_latent, w_mesh_in, preferred_element_type=jnp.float32) + jnp.dot(summed, w_message_in, preferred_element_type=jnp.float32) + mesh_bias
    mesh_hidden = jax.nn.silu(mesh_pre).astype(jnp.bfloat16)
    mesh_sum = group_sum(mesh_hidden, w_mesh_out) + mesh_out_bias
    mesh_out = (mesh_latent.astype(jnp.float32) + normalize(mesh_sum, mesh_gain, mesh_shift)).astype(jnp.bfloat16)
    return (mesh_out, edge_out)
```

```python
import functools

import jax
import jax.numpy as jnp
from jax import lax
from jax.experimental import pallas as pl
from jax.experimental.pallas import tpu as pltpu
from jax.sharding import PartitionSpec as P

EPSILON = 1e-05
CHUNKS = 2


def row_block(rows, most):
    block = most
    while rows % block:
        block //= 2
    return block


def norm_own(total, gain, offset):
    width = total.shape[1]
    own = gain.shape[1]
    center = jnp.sum(total, axis=1, keepdims=True) / width
    centered = total - center
    spread = jnp.sum(centered * centered, axis=1, keepdims=True) / width
    return centered[:, :own] * lax.rsqrt(spread + EPSILON) * gain + offset


def own_columns(column, latent, own, block, first):
    if own % 128 == 0:
        return latent, pl.BlockSpec((block, own), lambda i, c: (i + first, c[0]))
    cut = lax.dynamic_slice_in_dim(latent, column[0] * own, own, 1)
    return cut, pl.BlockSpec((block, own), lambda i, c: (i + first, 0))


def edge_kernel(column, hidden_ref, latent_ref, live_ref, w_ref, bias_ref, gain_ref, shift_ref, message_ref, out_ref):
    total = jnp.dot(hidden_ref[...], w_ref[...], preferred_element_type=jnp.float32) + bias_ref[...]
    message = norm_own(total, gain_ref[...], shift_ref[...]) * live_ref[...]
    message_ref[...] = message
    out_ref[...] = (latent_ref[...].astype(jnp.float32) + message).astype(out_ref.dtype)


def edge_finish(column, hidden, latent, first_row, live, w_out, bias, gain, shift):
    rows, full = hidden.shape
    own = gain.shape[1]
    block = row_block(rows, 1024)
    first = first_row // block
    latent, latent_spec = own_columns(column, latent, own, block, first)
    return pl.pallas_call(
        edge_kernel,
        grid_spec=pltpu.PrefetchScalarGridSpec(
            num_scalar_prefetch=1,
            grid=(rows // block,),
            in_specs=[
                pl.BlockSpec((block, full), lambda i, c: (i, 0)),
                latent_spec,
                pl.BlockSpec((block, 1), lambda i, c: (i + first, 0)),
                pl.BlockSpec((full, full), lambda i, c: (0, 0)),
                pl.BlockSpec((1, full), lambda i, c: (0, 0)),
                pl.BlockSpec((1, own), lambda i, c: (0, 0)),
                pl.BlockSpec((1, own), lambda i, c: (0, 0)),
            ],
            out_specs=[
                pl.BlockSpec((block, own), lambda i, c: (i, 0)),
                pl.BlockSpec((block, own), lambda i, c: (i, 0)),
            ],
        ),
        out_shape=[
            jax.ShapeDtypeStruct((rows, own), jnp.float32),
            jax.ShapeDtypeStruct((rows, own), jnp.bfloat16),
        ],
        cost_estimate=pl.CostEstimate(
            flops=2 * rows * full * full, bytes_accessed=2 * rows * full + 8 * rows * own, transcendentals=0
        ),
        name="edge_finish",
    )(column, hidden, latent, live, w_out, bias, gain, shift)


def mesh_kernel(column, latent_ref, own_ref, summed_ref, w_in_ref, w_msg_ref, bias_in_ref, w_out_ref, bias_ref, gain_ref, shift_ref, out_ref):
    pre = jnp.dot(latent_ref[...], w_in_ref[...], preferred_element_type=jnp.float32)
    pre = pre + jnp.dot(summed_ref[...], w_msg_ref[...], preferred_element_type=jnp.float32) + bias_in_ref[...]
    hidden = jax.nn.silu(pre).astype(jnp.bfloat16)
    total = jnp.dot(hidden, w_out_ref[...], preferred_element_type=jnp.float32) + bias_ref[...]
    update = norm_own(total, gain_ref[...], shift_ref[...])
    out_ref[...] = (own_ref[...].astype(jnp.float32) + update).astype(out_ref.dtype)


def mesh_finish(column, latent, summed, w_in, w_msg, bias_in, w_out, bias, gain, shift):
    rows, full = latent.shape
    own = gain.shape[1]
    block = row_block(rows, 1024)
    whole = lambda i, c: (0, 0)
    own_latent, own_spec = own_columns(column, latent, own, block, 0)
    return pl.pallas_call(
        mesh_kernel,
        grid_spec=pltpu.PrefetchScalarGridSpec(
            num_scalar_prefetch=1,
            grid=(rows // block,),
            in_specs=[
                pl.BlockSpec((block, full), lambda i, c: (i, 0)),
                own_spec,
                pl.BlockSpec((block, full), lambda i, c: (i, 0)),
                pl.BlockSpec((full, full), whole),
                pl.BlockSpec((full, full), whole),
                pl.BlockSpec((1, full), whole),
                pl.BlockSpec((full, full), whole),
                pl.BlockSpec((1, full), whole),
                pl.BlockSpec((1, own), whole),
                pl.BlockSpec((1, own), whole),
            ],
            out_specs=pl.BlockSpec((block, own), lambda i, c: (i, 0)),
        ),
        out_shape=jax.ShapeDtypeStruct((rows, own), jnp.bfloat16),
        cost_estimate=pl.CostEstimate(
            flops=6 * rows * full * full, bytes_accessed=4 * rows * full + 4 * rows * own, transcendentals=rows * full
        ),
        name="mesh_finish",
    )(column, latent, own_latent, summed, w_in, w_msg, bias_in, w_out, bias, gain, shift)


def pieces(x, size):
    return [x] + [
        lax.ppermute(x, "hidden", [((j + k) % size, j) for j in range(size)]) for k in range(1, size)
    ]


def turned(x, shift, axis):
    return lax.dynamic_slice_in_dim(jnp.concatenate([x, x], axis), shift, x.shape[axis], axis)


def shards(
    hidden_size,
    grid_latent,
    mesh_latent,
    edge_latent,
    senders,
    receivers,
    mesh_slot,
    edge_counts,
    w_edge,
    w_sender,
    w_receiver,
    edge_bias,
    w_edge_out,
    edge_out_bias,
    edge_gain,
    edge_shift,
    w_mesh_in,
    w_message_in,
    mesh_bias,
    w_mesh_out,
    mesh_out_bias,
    mesh_gain,
    mesh_shift,
):
    patch_index = lax.axis_index("patch")
    column_index = lax.axis_index("hidden")
    own_grid = grid_latent.shape[0]
    own_edges = edge_latent.shape[0]
    width = w_edge.shape[1]
    full = w_edge.shape[0]
    mesh_total = mesh_slot.shape[0]
    column = jnp.reshape(column_index, (1,)).astype(jnp.int32)

    receiver_part = jnp.dot(mesh_latent, w_receiver, preferred_element_type=jnp.float32).astype(
        jnp.bfloat16
    )
    table = lax.all_gather(receiver_part, "patch", axis=0, tiled=True)

    outer = pieces(jnp.concatenate([w_edge_out, w_mesh_out], 0), hidden_size)
    inner = pieces(jnp.concatenate([w_mesh_in, w_message_in], 0), hidden_size)
    biases = jnp.concatenate(pieces(jnp.stack([edge_out_bias, mesh_bias, mesh_out_bias]), hidden_size), 1)
    to_first = lax.rem(hidden_size - column_index, hidden_size)
    edge_w_out = jnp.concatenate([part[:width] for part in outer], 0)
    edge_w_out = turned(turned(edge_w_out, to_first * width, 0), column_index * width, 1)
    mesh_w_out = turned(jnp.concatenate([part[width:] for part in outer], 0), column_index * width, 1)
    mesh_w_in = jnp.concatenate([part[:full] for part in inner], 1)
    mesh_w_msg = jnp.concatenate([part[full:] for part in inner], 1)

    target_rows = jnp.take(mesh_slot, receivers)
    sender_local = senders - patch_index * own_grid
    live = (jnp.arange(own_edges, dtype=jnp.int32) < edge_counts[0]).astype(jnp.float32)[:, None]
    sender_part = jnp.dot(grid_latent, w_sender, preferred_element_type=jnp.float32)
    sent = jnp.take(sender_part, sender_local, axis=0)

    step = own_edges // CHUNKS
    spread_sums = jnp.zeros((mesh_total, width), jnp.float32)
    edge_outs = []
    for at in range(0, own_edges, step):
        rows = slice(at, at + step)
        edge_pre = (
            jnp.dot(edge_latent[rows], w_edge, preferred_element_type=jnp.float32)
            + sent[rows]
            + jnp.take(table, target_rows[rows], axis=0).astype(jnp.float32)
            + edge_bias
        )
        edge_hidden = jax.nn.silu(edge_pre).astype(jnp.bfloat16)
        gathered_hidden = lax.all_gather(edge_hidden, "hidden", axis=1, tiled=True)
        message, edge_out = edge_finish(
            column,
            gathered_hidden,
            edge_latent,
            at,
            live,
            edge_w_out,
            biases[:1],
            edge_gain[None],
            edge_shift[None],
        )
        edge_outs.append(edge_out)
        spread_sums = spread_sums.at[target_rows[rows]].add(message)
    edge_out = jnp.concatenate(edge_outs, 0)

    received = lax.psum_scatter(
        spread_sums.astype(jnp.bfloat16), "patch", scatter_dimension=0, tiled=True
    )
    gathered = lax.all_gather(received, "hidden", axis=1, tiled=True)
    mesh_out = mesh_finish(
        column,
        mesh_latent,
        gathered,
        mesh_w_in,
        mesh_w_msg,
        biases[1:2],
        mesh_w_out,
        biases[2:3],
        mesh_gain[None],
        mesh_shift[None],
    )
    return (mesh_out, edge_out)


def solution(mesh):
    return jax.shard_map(
        functools.partial(shards, mesh.shape["hidden"]),
        mesh=mesh,
        in_specs=(
            P("patch", None),
            P("patch", None),
            P("patch", None),
            P("patch"),
            P("patch"),
            P(),
            P("patch"),
            P(None, "hidden"),
            P(None, "hidden"),
            P(None, "hidden"),
            P("hidden"),
            P("hidden", None),
            P("hidden"),
            P("hidden"),
            P("hidden"),
            P(None, "hidden"),
            P(None, "hidden"),
            P("hidden"),
            P("hidden", None),
            P("hidden"),
            P("hidden"),
            P("hidden"),
        ),
        out_specs=(P("patch", "hidden"), P("patch", "hidden")),
        check_vma=False,
    )
```

```python
import functools

import jax
import jax.numpy as jnp
from jax import lax
from jax.experimental import pallas as pl
from jax.experimental.pallas import tpu as pltpu
from jax.sharding import PartitionSpec as P

EPSILON = 1e-05
CHUNKS = 2


def row_block(rows, most):
    block = most
    while rows % block:
        block //= 2
    return block


def norm_own(total, gain, offset):
    width = total.shape[1]
    own = gain.shape[1]
    center = jnp.sum(total, axis=1, keepdims=True) / width
    centered = total - center
    spread = jnp.sum(centered * centered, axis=1, keepdims=True) / width
    return centered[:, :own] * lax.rsqrt(spread + EPSILON) * gain + offset


def own_columns(column, latent, own, block, first):
    if own % 128 == 0:
        return latent, pl.BlockSpec((block, own), lambda i, c: (i + first, c[0]))
    cut = lax.dynamic_slice_in_dim(latent, column[0] * own, own, 1)
    return cut, pl.BlockSpec((block, own), lambda i, c: (i + first, 0))


def edge_kernel(column, hidden_ref, latent_ref, live_ref, w_ref, bias_ref, gain_ref, shift_ref, message_ref, out_ref):
    total = jnp.dot(hidden_ref[...], w_ref[...], preferred_element_type=jnp.float32) + bias_ref[...]
    message = norm_own(total, gain_ref[...], shift_ref[...]) * live_ref[...]
    message_ref[...] = message
    out_ref[...] = (latent_ref[...].astype(jnp.float32) + message).astype(out_ref.dtype)


def edge_finish(column, hidden, latent, first_row, live, w_out, bias, gain, shift):
    rows, full = hidden.shape
    own = gain.shape[1]
    block = row_block(rows, 1024)
    first = first_row // block
    latent, latent_spec = own_columns(column, latent, own, block, first)
    return pl.pallas_call(
        edge_kernel,
        grid_spec=pltpu.PrefetchScalarGridSpec(
            num_scalar_prefetch=1,
            grid=(rows // block,),
            in_specs=[
                pl.BlockSpec((block, full), lambda i, c: (i, 0)),
                latent_spec,
                pl.BlockSpec((block, 1), lambda i, c: (i + first, 0)),
                pl.BlockSpec((full, full), lambda i, c: (0, 0)),
                pl.BlockSpec((1, full), lambda i, c: (0, 0)),
                pl.BlockSpec((1, own), lambda i, c: (0, 0)),
                pl.BlockSpec((1, own), lambda i, c: (0, 0)),
            ],
            out_specs=[
                pl.BlockSpec((block, own), lambda i, c: (i, 0)),
                pl.BlockSpec((block, own), lambda i, c: (i, 0)),
            ],
        ),
        out_shape=[
            jax.ShapeDtypeStruct((rows, own), jnp.float32),
            jax.ShapeDtypeStruct((rows, own), jnp.bfloat16),
        ],
        cost_estimate=pl.CostEstimate(
            flops=2 * rows * full * full, bytes_accessed=2 * rows * full + 8 * rows * own, transcendentals=0
        ),
        name="edge_finish",
    )(column, hidden, latent, live, w_out, bias, gain, shift)


def mesh_kernel(column, latent_ref, own_ref, summed_ref, w_in_ref, w_msg_ref, bias_in_ref, w_out_ref, bias_ref, gain_ref, shift_ref, out_ref):
    pre = jnp.dot(latent_ref[...], w_in_ref[...], preferred_element_type=jnp.float32)
    summed = jnp.concatenate([summed_ref[h] for h in range(summed_ref.shape[0])], axis=1)
    pre = pre + jnp.dot(summed, w_msg_ref[...], preferred_element_type=jnp.float32) + bias_in_ref[...]
    hidden = jax.nn.silu(pre).astype(jnp.bfloat16)
    total = jnp.dot(hidden, w_out_ref[...], preferred_element_type=jnp.float32) + bias_ref[...]
    update = norm_own(total, gain_ref[...], shift_ref[...])
    out_ref[...] = (own_ref[...].astype(jnp.float32) + update).astype(out_ref.dtype)


def mesh_finish(column, latent, summed, w_in, w_msg, bias_in, w_out, bias, gain, shift):
    rows, full = latent.shape
    own = gain.shape[1]
    block = row_block(rows, 1024)
    whole = lambda i, c: (0, 0)
    own_latent, own_spec = own_columns(column, latent, own, block, 0)
    return pl.pallas_call(
        mesh_kernel,
        grid_spec=pltpu.PrefetchScalarGridSpec(
            num_scalar_prefetch=1,
            grid=(rows // block,),
            in_specs=[
                pl.BlockSpec((block, full), lambda i, c: (i, 0)),
                own_spec,
                pl.BlockSpec((summed.shape[0], block, summed.shape[2]), lambda i, c: (0, i, 0)),
                pl.BlockSpec((full, full), whole),
                pl.BlockSpec((full, full), whole),
                pl.BlockSpec((1, full), whole),
                pl.BlockSpec((full, full), whole),
                pl.BlockSpec((1, full), whole),
                pl.BlockSpec((1, own), whole),
                pl.BlockSpec((1, own), whole),
            ],
            out_specs=pl.BlockSpec((block, own), lambda i, c: (i, 0)),
        ),
        out_shape=jax.ShapeDtypeStruct((rows, own), jnp.bfloat16),
        cost_estimate=pl.CostEstimate(
            flops=6 * rows * full * full, bytes_accessed=4 * rows * full + 4 * rows * own, transcendentals=rows * full
        ),
        name="mesh_finish",
    )(column, latent, own_latent, summed, w_in, w_msg, bias_in, w_out, bias, gain, shift)


def combine_kernel(sizes, part_ref, out_ref, own, paired, crossed, gathered, own_sem, pair_send, pair_recv, cross_send, cross_recv, side_send, side_recv, far_send, far_recv, relay_send, relay_recv, out_sem):
    outer_size, far_size, chunks, rows = sizes
    patch, rank = lax.axis_index("patch"), lax.axis_index("hidden")
    outer, inner = patch // 2, patch % 2
    far, side = rank // 2, rank % 2
    pair_peer = outer * 2 + (1 - inner)
    side_peer = far * 2 + (1 - side)
    shift = lambda at, by, size: lax.rem(at + by, size)
    cross_peers = [shift(outer, k + 1, outer_size) * 2 + inner for k in range(outer_size - 1)]
    far_peers = [shift(far, k + 1, far_size) * 2 + side for k in range(far_size - 1)]
    blocks = [shift(outer, k + 1, outer_size) for k in range(outer_size)]

    barrier = pltpu.get_barrier_semaphore()
    for peer in [pair_peer] + cross_peers:
        pl.semaphore_signal(barrier, inc=1, device_id={"patch": peer}, device_id_type=pl.DeviceIdType.MESH)
    for peer in [side_peer] + far_peers:
        pl.semaphore_signal(barrier, inc=1, device_id={"hidden": peer}, device_id_type=pl.DeviceIdType.MESH)
    pl.semaphore_wait(barrier, outer_size + far_size)

    def send(src, dst, send_sem, recv_sem, axis, peer):
        copy = pltpu.make_async_remote_copy(
            src_ref=src,
            dst_ref=dst,
            send_sem=send_sem,
            recv_sem=recv_sem,
            device_id={axis: peer},
            device_id_type=pl.DeviceIdType.MESH,
        )
        copy.start()
        return copy

    def span(c):
        return pl.ds(c * rows, rows)

    loads, pairs, crosses, sides, fars, relays, outs = [], {}, {}, {}, {}, {}, []
    for c in range(chunks):
        load = pltpu.make_async_copy(part_ref.at[:, inner, span(c)], own.at[c], own_sem.at[c])
        load.start()
        loads.append(load)
        for k in range(outer_size):
            pairs[c, k] = send(
                part_ref.at[blocks[k], 1 - inner, span(c)],
                paired.at[c, k],
                pair_send.at[c, k],
                pair_recv.at[c, k],
                "patch",
                pair_peer,
            )

    tile = row_block(rows, 128)

    def reduce_pair(c):
        loads[c].wait()
        for k in range(outer_size - 1):
            pairs[c, k].wait_recv()

            def add(i, carry):
                at = pl.ds(pl.multiple_of(i * tile, tile), tile)
                total = own[c, blocks[k], at].astype(jnp.float32) + paired[c, k, at].astype(jnp.float32)
                own[c, blocks[k], at] = total.astype(jnp.bfloat16)
                return carry

            lax.fori_loop(0, rows // tile, add, 0)
            crosses[c, k] = send(
                own.at[c, blocks[k]],
                crossed.at[c, k],
                cross_send.at[c, k],
                cross_recv.at[c, k],
                "patch",
                cross_peers[k],
            )
        pairs[c, outer_size - 1].wait_recv()

    def emit(c, source, sem):
        copy = pltpu.make_async_copy(gathered.at[c, source], out_ref.at[source, span(c)], sem)
        copy.start()
        outs.append(copy)

    def finish(c):
        for k in range(outer_size - 1):
            crosses[c, k].wait_recv()

        def add(i, carry):
            at = pl.ds(pl.multiple_of(i * tile, tile), tile)
            total = own[c, outer, at].astype(jnp.float32) + paired[c, outer_size - 1, at].astype(jnp.float32)
            for k in range(outer_size - 1):
                total = total + crossed[c, k, at].astype(jnp.float32)
            gathered[c, rank, at] = total.astype(jnp.bfloat16)
            return carry

        lax.fori_loop(0, rows // tile, add, 0)
        mine = gathered.at[c, rank]
        for k in range(far_size - 1):
            fars[c, k] = send(mine, mine, far_send.at[c, k], far_recv.at[c, k], "hidden", far_peers[k])
        sides[c] = send(mine, mine, side_send.at[c], side_recv.at[c], "hidden", side_peer)
        emit(c, rank, out_sem.at[c, 0])

    def relay(c):
        for k in range(far_size - 1):
            fars[c, k].wait_recv()
            source = shift(far, far_size - 1 - k, far_size) * 2 + side
            block = gathered.at[c, source]
            relays[c, k] = send(block, block, relay_send.at[c, k], relay_recv.at[c, k], "hidden", side_peer)
            emit(c, source, out_sem.at[c, 1 + k])

    def collect(c):
        sides[c].wait_recv()
        emit(c, side_peer, out_sem.at[c, far_size])
        for k in range(far_size - 1):
            relays[c, k].wait_recv()
            source = shift(far, far_size - 1 - k, far_size) * 2 + (1 - side)
            emit(c, source, out_sem.at[c, far_size + 1 + k])

    for c in range(chunks + 3):
        if c < chunks:
            reduce_pair(c)
        if 0 <= c - 1 < chunks:
            finish(c - 1)
        if 0 <= c - 2 < chunks:
            relay(c - 2)
        if 0 <= c - 3 < chunks:
            collect(c - 3)
    for group in (pairs, crosses, sides, fars, relays):
        for copy in group.values():
            copy.wait_send()
    for copy in outs:
        copy.wait()


def combine(parts, patches, ranks):
    total_rows, width = parts.shape
    rows = total_rows // patches
    outer_size, far_size = patches // 2, ranks // 2
    chunks = 5 if rows % 80 == 0 else 4
    size = rows // chunks
    dma = pltpu.SemaphoreType.DMA
    cross = (chunks, outer_size - 1)
    far = (chunks, far_size - 1)
    return pl.pallas_call(
        functools.partial(combine_kernel, (outer_size, far_size, chunks, size)),
        in_specs=[pl.BlockSpec(memory_space=pl.ANY)],
        out_specs=pl.BlockSpec(memory_space=pl.ANY),
        out_shape=jax.ShapeDtypeStruct((ranks, rows, width), jnp.bfloat16),
        scratch_shapes=[
            pltpu.VMEM((chunks, outer_size, size, width), jnp.bfloat16),
            pltpu.VMEM((chunks, outer_size, size, width), jnp.bfloat16),
            pltpu.VMEM(cross + (size, width), jnp.bfloat16),
            pltpu.VMEM((chunks, ranks, size, width), jnp.bfloat16),
            dma((chunks,)),
            dma((chunks, outer_size)),
            dma((chunks, outer_size)),
            dma(cross),
            dma(cross),
            dma((chunks,)),
            dma((chunks,)),
            dma(far),
            dma(far),
            dma(far),
            dma(far),
            dma((chunks, ranks)),
        ],
        compiler_params=pltpu.CompilerParams(
            collective_id=0, has_side_effects=True, vmem_limit_bytes=48 * 1024 * 1024
        ),
        name="combine",
    )(parts.reshape(outer_size, 2, rows, width))


def pieces(x, size):
    return [x] + [
        lax.ppermute(x, "hidden", [((j + k) % size, j) for j in range(size)]) for k in range(1, size)
    ]


def rows_at(x, index):
    return x.at[index].get(mode="promise_in_bounds")


def turned(x, shift, axis):
    return lax.dynamic_slice_in_dim(jnp.concatenate([x, x], axis), shift, x.shape[axis], axis)


def shards(
    patches,
    hidden_size,
    grid_latent,
    mesh_latent,
    edge_latent,
    senders,
    receivers,
    mesh_slot,
    edge_counts,
    w_edge,
    w_sender,
    w_receiver,
    edge_bias,
    w_edge_out,
    edge_out_bias,
    edge_gain,
    edge_shift,
    w_mesh_in,
    w_message_in,
    mesh_bias,
    w_mesh_out,
    mesh_out_bias,
    mesh_gain,
    mesh_shift,
):
    patch_index = lax.axis_index("patch")
    column_index = lax.axis_index("hidden")
    own_grid = grid_latent.shape[0]
    own_edges = edge_latent.shape[0]
    width = w_edge.shape[1]
    full = w_edge.shape[0]
    mesh_total = mesh_slot.shape[0]
    column = jnp.reshape(column_index, (1,)).astype(jnp.int32)

    receiver_part = jnp.dot(mesh_latent, w_receiver, preferred_element_type=jnp.float32).astype(
        jnp.bfloat16
    )
    table = lax.all_gather(receiver_part, "patch", axis=0, tiled=True)

    outer = pieces(jnp.concatenate([w_edge_out, w_mesh_out], 0), hidden_size)
    inner = pieces(jnp.concatenate([w_mesh_in, w_message_in], 0), hidden_size)
    biases = jnp.concatenate(pieces(jnp.stack([edge_out_bias, mesh_bias, mesh_out_bias]), hidden_size), 1)
    to_first = lax.rem(hidden_size - column_index, hidden_size)
    edge_w_out = jnp.concatenate([part[:width] for part in outer], 0)
    edge_w_out = turned(turned(edge_w_out, to_first * width, 0), column_index * width, 1)
    mesh_w_out = turned(jnp.concatenate([part[width:] for part in outer], 0), column_index * width, 1)
    mesh_w_in = jnp.concatenate([part[:full] for part in inner], 1)
    mesh_w_msg = jnp.concatenate([part[full:] for part in inner], 1)

    target_rows = rows_at(mesh_slot, receivers)
    weights = (edge_w_out, mesh_w_out, mesh_w_in, mesh_w_msg, biases)
    target_rows, weights = lax.optimization_barrier((target_rows, weights))
    edge_w_out, mesh_w_out, mesh_w_in, mesh_w_msg, biases = weights
    sender_local = senders - patch_index * own_grid
    live = (jnp.arange(own_edges, dtype=jnp.int32) < edge_counts[0]).astype(jnp.float32)[:, None]
    sender_part = jnp.dot(grid_latent, w_sender, preferred_element_type=jnp.float32)
    sent = rows_at(sender_part, sender_local)

    step = own_edges // CHUNKS
    spread_sums = jnp.zeros((mesh_total, width), jnp.float32)
    edge_outs = []
    for at in range(0, own_edges, step):
        rows = slice(at, at + step)
        edge_pre = (
            jnp.dot(edge_latent[rows], w_edge, preferred_element_type=jnp.float32)
            + sent[rows]
            + rows_at(table, target_rows[rows]).astype(jnp.float32)
            + edge_bias
        )
        edge_hidden = jax.nn.silu(edge_pre).astype(jnp.bfloat16)
        gathered_hidden = lax.all_gather(edge_hidden, "hidden", axis=1, tiled=True)
        message, edge_out = edge_finish(
            column,
            gathered_hidden,
            edge_latent,
            at,
            live,
            edge_w_out,
            biases[:1],
            edge_gain[None],
            edge_shift[None],
        )
        edge_outs.append(edge_out)
        spread_sums = spread_sums.at[target_rows[rows]].add(message, mode="promise_in_bounds")
    edge_out = jnp.concatenate(edge_outs, 0)

    spread_sums = spread_sums.astype(jnp.bfloat16)
    if width % 128 == 0 and patches % 2 == 0 and patches > 2 and hidden_size % 2 == 0 and hidden_size > 2:
        gathered = combine(spread_sums, patches, hidden_size)
    else:
        received = lax.psum_scatter(spread_sums, "patch", scatter_dimension=0, tiled=True)
        gathered = lax.all_gather(received, "hidden", axis=1, tiled=True)[None]
    mesh_out = mesh_finish(
        column,
        mesh_latent,
        gathered,
        mesh_w_in,
        mesh_w_msg,
        biases[1:2],
        mesh_w_out,
        biases[2:3],
        mesh_gain[None],
        mesh_shift[None],
    )
    return (mesh_out, edge_out)


def solution(mesh):
    return jax.shard_map(
        functools.partial(shards, mesh.shape["patch"], mesh.shape["hidden"]),
        mesh=mesh,
        in_specs=(
            P("patch", None),
            P("patch", None),
            P("patch", None),
            P("patch"),
            P("patch"),
            P(),
            P("patch"),
            P(None, "hidden"),
            P(None, "hidden"),
            P(None, "hidden"),
            P("hidden"),
            P("hidden", None),
            P("hidden"),
            P("hidden"),
            P("hidden"),
            P(None, "hidden"),
            P(None, "hidden"),
            P("hidden"),
            P("hidden", None),
            P("hidden"),
            P("hidden"),
            P("hidden"),
        ),
        out_specs=(P("patch", "hidden"), P("patch", "hidden")),
        check_vma=False,
    )
```

```python
import functools

import jax
import jax.numpy as jnp
from jax import lax
from jax.experimental import pallas as pl
from jax.experimental.pallas import tpu as pltpu
from jax.sharding import PartitionSpec as P

EPSILON = 1e-05
CHUNKS = 2


def row_block(rows, most):
    block = most
    while rows % block:
        block //= 2
    return block


def norm_own(total, gain, offset):
    width = total.shape[1]
    own = gain.shape[1]
    center = jnp.sum(total, axis=1, keepdims=True) / width
    centered = total - center
    spread = jnp.sum(centered * centered, axis=1, keepdims=True) / width
    return centered[:, :own] * lax.rsqrt(spread + EPSILON) * gain + offset


def own_columns(column, latent, own, block, first):
    if own % 128 == 0:
        return latent, pl.BlockSpec((block, own), lambda i, c: (i + first, c[0]))
    cut = lax.dynamic_slice_in_dim(latent, column[0] * own, own, 1)
    return cut, pl.BlockSpec((block, own), lambda i, c: (i + first, 0))


def edge_kernel(first_row, scalars, hidden_ref, latent_ref, w_ref, bias_ref, gain_ref, shift_ref, message_ref, out_ref):
    total = jnp.dot(hidden_ref[...], w_ref[...], preferred_element_type=jnp.float32) + bias_ref[...]
    start = first_row + pl.program_id(0) * total.shape[0]
    slot = start + lax.broadcasted_iota(jnp.int32, message_ref.shape, 0)
    message = norm_own(total, gain_ref[...], shift_ref[...])
    message = jnp.where(slot < scalars[1], message, 0.0)
    message_ref[...] = message
    out_ref[...] = (latent_ref[...].astype(jnp.float32) + message).astype(out_ref.dtype)


def edge_finish(column, hidden, latent, first_row, w_out, bias, gain, shift):
    rows, full = hidden.shape
    own = gain.shape[1]
    block = row_block(rows, 1024)
    first = first_row // block
    latent, latent_spec = own_columns(column, latent, own, block, first)
    return pl.pallas_call(
        functools.partial(edge_kernel, first_row),
        grid_spec=pltpu.PrefetchScalarGridSpec(
            num_scalar_prefetch=1,
            grid=(rows // block,),
            in_specs=[
                pl.BlockSpec((block, full), lambda i, c: (i, 0)),
                latent_spec,
                pl.BlockSpec((full, full), lambda i, c: (0, 0)),
                pl.BlockSpec((1, full), lambda i, c: (0, 0)),
                pl.BlockSpec((1, own), lambda i, c: (0, 0)),
                pl.BlockSpec((1, own), lambda i, c: (0, 0)),
            ],
            out_specs=[
                pl.BlockSpec((block, own), lambda i, c: (i, 0)),
                pl.BlockSpec((block, own), lambda i, c: (i, 0)),
            ],
        ),
        out_shape=[
            jax.ShapeDtypeStruct((rows, own), jnp.float32),
            jax.ShapeDtypeStruct((rows, own), jnp.bfloat16),
        ],
        cost_estimate=pl.CostEstimate(
            flops=2 * rows * full * full, bytes_accessed=2 * rows * full + 8 * rows * own, transcendentals=0
        ),
        name="edge_finish",
    )(column, hidden, latent, w_out, bias, gain, shift)


def mesh_kernel(column, latent_ref, own_ref, summed_ref, w_in_ref, w_msg_ref, bias_in_ref, w_out_ref, bias_ref, gain_ref, shift_ref, out_ref):
    pre = jnp.dot(latent_ref[...], w_in_ref[...], preferred_element_type=jnp.float32)
    summed = jnp.concatenate([summed_ref[h] for h in range(summed_ref.shape[0])], axis=1)
    pre = pre + jnp.dot(summed, w_msg_ref[...], preferred_element_type=jnp.float32) + bias_in_ref[...]
    hidden = jax.nn.silu(pre).astype(jnp.bfloat16)
    total = jnp.dot(hidden, w_out_ref[...], preferred_element_type=jnp.float32) + bias_ref[...]
    update = norm_own(total, gain_ref[...], shift_ref[...])
    out_ref[...] = (own_ref[...].astype(jnp.float32) + update).astype(out_ref.dtype)


def mesh_finish(column, latent, summed, w_in, w_msg, bias_in, w_out, bias, gain, shift):
    rows, full = latent.shape
    own = gain.shape[1]
    block = row_block(rows, 1024)
    whole = lambda i, c: (0, 0)
    own_latent, own_spec = own_columns(column, latent, own, block, 0)
    return pl.pallas_call(
        mesh_kernel,
        grid_spec=pltpu.PrefetchScalarGridSpec(
            num_scalar_prefetch=1,
            grid=(rows // block,),
            in_specs=[
                pl.BlockSpec((block, full), lambda i, c: (i, 0)),
                own_spec,
                pl.BlockSpec((summed.shape[0], block, summed.shape[2]), lambda i, c: (0, i, 0)),
                pl.BlockSpec((full, full), whole),
                pl.BlockSpec((full, full), whole),
                pl.BlockSpec((1, full), whole),
                pl.BlockSpec((full, full), whole),
                pl.BlockSpec((1, full), whole),
                pl.BlockSpec((1, own), whole),
                pl.BlockSpec((1, own), whole),
            ],
            out_specs=pl.BlockSpec((block, own), lambda i, c: (i, 0)),
        ),
        out_shape=jax.ShapeDtypeStruct((rows, own), jnp.bfloat16),
        cost_estimate=pl.CostEstimate(
            flops=6 * rows * full * full, bytes_accessed=4 * rows * full + 4 * rows * own, transcendentals=rows * full
        ),
        name="mesh_finish",
    )(column, latent, own_latent, summed, w_in, w_msg, bias_in, w_out, bias, gain, shift)


def combine_kernel(sizes, part_ref, out_ref, stage, leaving, own, paired, crossed, gathered, own_sem, pair_send, pair_recv, cross_send, cross_recv, side_send, side_recv, far_send, far_recv, relay_send, relay_recv, out_sem):
    outer_size, far_size, chunks, rows = sizes
    patch, rank = lax.axis_index("patch"), lax.axis_index("hidden")
    outer, inner = patch // 2, patch % 2
    far, side = rank // 2, rank % 2
    pair_peer = outer * 2 + (1 - inner)
    side_peer = far * 2 + (1 - side)
    shift = lambda at, by, size: lax.rem(at + by, size)
    cross_peers = [shift(outer, k + 1, outer_size) * 2 + inner for k in range(outer_size - 1)]
    far_peers = [shift(far, k + 1, far_size) * 2 + side for k in range(far_size - 1)]
    blocks = [shift(outer, k + 1, outer_size) for k in range(outer_size)]

    barrier = pltpu.get_barrier_semaphore()
    for peer in [pair_peer] + cross_peers:
        pl.semaphore_signal(barrier, inc=1, device_id={"patch": peer}, device_id_type=pl.DeviceIdType.MESH)
    for peer in [side_peer] + far_peers:
        pl.semaphore_signal(barrier, inc=1, device_id={"hidden": peer}, device_id_type=pl.DeviceIdType.MESH)
    pl.semaphore_wait(barrier, outer_size + far_size)

    def send(src, dst, send_sem, recv_sem, axis, peer):
        copy = pltpu.make_async_remote_copy(
            src_ref=src,
            dst_ref=dst,
            send_sem=send_sem,
            recv_sem=recv_sem,
            device_id={axis: peer},
            device_id_type=pl.DeviceIdType.MESH,
        )
        copy.start()
        return copy

    def span(c):
        return pl.ds(c * rows, rows)

    loads, pairs, crosses, sides, fars, relays, outs = [], {}, {}, {}, {}, {}, []
    tile = row_block(rows, 128)

    def load(c):
        copy = pltpu.make_async_copy(part_ref.at[:, :, span(c)], stage.at[c % 2], own_sem.at[c])
        copy.start()
        loads.append(copy)

    load(0)
    load(1)
    for c in range(chunks):
        loads[c].wait()

        def narrow(i, carry):
            at = pl.ds(pl.multiple_of(i * tile, tile), tile)
            for block in range(outer_size):
                own[c, block, at] = stage[c % 2, block, inner, at].astype(jnp.bfloat16)
                leaving[c, block, at] = stage[c % 2, block, 1 - inner, at].astype(jnp.bfloat16)
            return carry

        lax.fori_loop(0, rows // tile, narrow, 0)
        if c + 2 < chunks:
            load(c + 2)
        for k in range(outer_size):
            pairs[c, k] = send(
                leaving.at[c, blocks[k]],
                paired.at[c, k],
                pair_send.at[c, k],
                pair_recv.at[c, k],
                "patch",
                pair_peer,
            )

    def reduce_pair(c):
        for k in range(outer_size - 1):
            pairs[c, k].wait_recv()

            def add(i, carry):
                at = pl.ds(pl.multiple_of(i * tile, tile), tile)
                total = own[c, blocks[k], at].astype(jnp.float32) + paired[c, k, at].astype(jnp.float32)
                own[c, blocks[k], at] = total.astype(jnp.bfloat16)
                return carry

            lax.fori_loop(0, rows // tile, add, 0)
            crosses[c, k] = send(
                own.at[c, blocks[k]],
                crossed.at[c, k],
                cross_send.at[c, k],
                cross_recv.at[c, k],
                "patch",
                cross_peers[k],
            )
        pairs[c, outer_size - 1].wait_recv()

    def emit(c, source, sem):
        copy = pltpu.make_async_copy(gathered.at[c, source], out_ref.at[source, span(c)], sem)
        copy.start()
        outs.append(copy)

    def finish(c):
        for k in range(outer_size - 1):
            crosses[c, k].wait_recv()

        def add(i, carry):
            at = pl.ds(pl.multiple_of(i * tile, tile), tile)
            total = own[c, outer, at].astype(jnp.float32) + paired[c, outer_size - 1, at].astype(jnp.float32)
            for k in range(outer_size - 1):
                total = total + crossed[c, k, at].astype(jnp.float32)
            gathered[c, rank, at] = total.astype(jnp.bfloat16)
            return carry

        lax.fori_loop(0, rows // tile, add, 0)
        mine = gathered.at[c, rank]
        for k in range(far_size - 1):
            fars[c, k] = send(mine, mine, far_send.at[c, k], far_recv.at[c, k], "hidden", far_peers[k])
        sides[c] = send(mine, mine, side_send.at[c], side_recv.at[c], "hidden", side_peer)
        emit(c, rank, out_sem.at[c, 0])

    def relay(c):
        for k in range(far_size - 1):
            fars[c, k].wait_recv()
            source = shift(far, far_size - 1 - k, far_size) * 2 + side
            block = gathered.at[c, source]
            relays[c, k] = send(block, block, relay_send.at[c, k], relay_recv.at[c, k], "hidden", side_peer)
            emit(c, source, out_sem.at[c, 1 + k])

    def collect(c):
        sides[c].wait_recv()
        emit(c, side_peer, out_sem.at[c, far_size])
        for k in range(far_size - 1):
            relays[c, k].wait_recv()
            source = shift(far, far_size - 1 - k, far_size) * 2 + (1 - side)
            emit(c, source, out_sem.at[c, far_size + 1 + k])

    for c in range(chunks + 3):
        if c < chunks:
            reduce_pair(c)
        if 0 <= c - 1 < chunks:
            finish(c - 1)
        if 0 <= c - 2 < chunks:
            relay(c - 2)
        if 0 <= c - 3 < chunks:
            collect(c - 3)
    for group in (pairs, crosses, sides, fars, relays):
        for copy in group.values():
            copy.wait_send()
    for copy in outs:
        copy.wait()


def combine(parts, patches, ranks):
    total_rows, width = parts.shape
    rows = total_rows // patches
    outer_size, far_size = patches // 2, ranks // 2
    chunks = 10 if rows % 160 == 0 else 4
    size = rows // chunks
    dma = pltpu.SemaphoreType.DMA
    cross = (chunks, outer_size - 1)
    far = (chunks, far_size - 1)
    return pl.pallas_call(
        functools.partial(combine_kernel, (outer_size, far_size, chunks, size)),
        in_specs=[pl.BlockSpec(memory_space=pl.ANY)],
        out_specs=pl.BlockSpec(memory_space=pl.ANY),
        out_shape=jax.ShapeDtypeStruct((ranks, rows, width), jnp.bfloat16),
        scratch_shapes=[
            pltpu.VMEM((2, outer_size, 2, size, width), jnp.float32),
            pltpu.VMEM((chunks, outer_size, size, width), jnp.bfloat16),
            pltpu.VMEM((chunks, outer_size, size, width), jnp.bfloat16),
            pltpu.VMEM((chunks, outer_size, size, width), jnp.bfloat16),
            pltpu.VMEM(cross + (size, width), jnp.bfloat16),
            pltpu.VMEM((chunks, ranks, size, width), jnp.bfloat16),
            dma((chunks,)),
            dma((chunks, outer_size)),
            dma((chunks, outer_size)),
            dma(cross),
            dma(cross),
            dma((chunks,)),
            dma((chunks,)),
            dma(far),
            dma(far),
            dma(far),
            dma(far),
            dma((chunks, ranks)),
        ],
        compiler_params=pltpu.CompilerParams(
            collective_id=0, has_side_effects=True, vmem_limit_bytes=48 * 1024 * 1024
        ),
        name="combine",
    )(parts.reshape(outer_size, 2, rows, width))


def pieces(x, size):
    return [x] + [
        lax.ppermute(x, "hidden", [((j + k) % size, j) for j in range(size)]) for k in range(1, size)
    ]


def rows_at(x, index):
    return x.at[index].get(mode="promise_in_bounds")


def turned(x, shift, axis):
    return lax.dynamic_slice_in_dim(jnp.concatenate([x, x], axis), shift, x.shape[axis], axis)


def shards(
    patches,
    hidden_size,
    grid_latent,
    mesh_latent,
    edge_latent,
    senders,
    receivers,
    mesh_slot,
    edge_counts,
    w_edge,
    w_sender,
    w_receiver,
    edge_bias,
    w_edge_out,
    edge_out_bias,
    edge_gain,
    edge_shift,
    w_mesh_in,
    w_message_in,
    mesh_bias,
    w_mesh_out,
    mesh_out_bias,
    mesh_gain,
    mesh_shift,
):
    patch_index = lax.axis_index("patch")
    column_index = lax.axis_index("hidden")
    own_grid = grid_latent.shape[0]
    own_edges = edge_latent.shape[0]
    width = w_edge.shape[1]
    full = w_edge.shape[0]
    mesh_total = mesh_slot.shape[0]
    column = jnp.stack([column_index.astype(jnp.int32), edge_counts[0]])

    receiver_part = jnp.dot(mesh_latent, w_receiver, preferred_element_type=jnp.float32).astype(
        jnp.bfloat16
    )
    table = lax.all_gather(receiver_part, "patch", axis=0, tiled=True)

    outer = pieces(jnp.concatenate([w_edge_out, w_mesh_out], 0), hidden_size)
    inner = pieces(jnp.concatenate([w_mesh_in, w_message_in], 0), hidden_size)
    biases = jnp.concatenate(pieces(jnp.stack([edge_out_bias, mesh_bias, mesh_out_bias]), hidden_size), 1)
    to_first = lax.rem(hidden_size - column_index, hidden_size)
    edge_w_out = jnp.concatenate([part[:width] for part in outer], 0)
    edge_w_out = turned(turned(edge_w_out, to_first * width, 0), column_index * width, 1)
    mesh_w_out = turned(jnp.concatenate([part[width:] for part in outer], 0), column_index * width, 1)
    mesh_w_in = jnp.concatenate([part[:full] for part in inner], 1)
    mesh_w_msg = jnp.concatenate([part[full:] for part in inner], 1)

    target_rows = rows_at(mesh_slot, receivers)
    weights = (edge_w_out, mesh_w_out, mesh_w_in, mesh_w_msg, biases)
    target_rows, weights = lax.optimization_barrier((target_rows, weights))
    edge_w_out, mesh_w_out, mesh_w_in, mesh_w_msg, biases = weights
    sender_local = senders - patch_index * own_grid
    sender_part = jnp.dot(grid_latent, w_sender, preferred_element_type=jnp.float32)
    sent = rows_at(sender_part, sender_local)

    step = own_edges // CHUNKS
    spread_sums = jnp.zeros((mesh_total, width), jnp.float32)
    edge_outs = []
    for at in range(0, own_edges, step):
        rows = slice(at, at + step)
        edge_pre = (
            jnp.dot(edge_latent[rows], w_edge, preferred_element_type=jnp.float32)
            + sent[rows]
            + rows_at(table, target_rows[rows]).astype(jnp.float32)
            + edge_bias
        )
        edge_hidden = jax.nn.silu(edge_pre).astype(jnp.bfloat16)
        gathered_hidden = lax.all_gather(edge_hidden, "hidden", axis=1, tiled=True)
        message, edge_out = edge_finish(
            column,
            gathered_hidden,
            edge_latent,
            at,
            edge_w_out,
            biases[:1],
            edge_gain[None],
            edge_shift[None],
        )
        edge_outs.append(edge_out)
        spread_sums = spread_sums.at[target_rows[rows]].add(message, mode="promise_in_bounds")
    edge_out = jnp.concatenate(edge_outs, 0)

    if width % 128 == 0 and patches % 2 == 0 and patches > 2 and hidden_size % 2 == 0 and hidden_size > 2:
        gathered = combine(spread_sums, patches, hidden_size)
    else:
        received = lax.psum_scatter(
            spread_sums.astype(jnp.bfloat16), "patch", scatter_dimension=0, tiled=True
        )
        gathered = lax.all_gather(received, "hidden", axis=1, tiled=True)[None]
    mesh_out = mesh_finish(
        column,
        mesh_latent,
        gathered,
        mesh_w_in,
        mesh_w_msg,
        biases[1:2],
        mesh_w_out,
        biases[2:3],
        mesh_gain[None],
        mesh_shift[None],
    )
    return (mesh_out, edge_out)


def solution(mesh):
    return jax.shard_map(
        functools.partial(shards, mesh.shape["patch"], mesh.shape["hidden"]),
        mesh=mesh,
        in_specs=(
            P("patch", None),
            P("patch", None),
            P("patch", None),
            P("patch"),
            P("patch"),
            P(),
            P("patch"),
            P(None, "hidden"),
            P(None, "hidden"),
            P(None, "hidden"),
            P("hidden"),
            P("hidden", None),
            P("hidden"),
            P("hidden"),
            P("hidden"),
            P(None, "hidden"),
            P(None, "hidden"),
            P("hidden"),
            P("hidden", None),
            P("hidden"),
            P("hidden"),
            P("hidden"),
        ),
        out_specs=(P("patch", "hidden"), P("patch", "hidden")),
        check_vma=False,
    )
```
